32 devices in a mesh: dp: 4 (over z), mp: 8 (over y, x, core).
Axes of the slice: x: 2, y: 2, z: 4, core: 2. Of those that a mesh axis runs over, the one named last changes fastest.
Arguments:
- weight: bfloat16 [5120, 32768], P('dp', 'mp'), may hold values from -0.078125 to 0.078125
- rank_map: int32 [8], replicated, may hold values from 0 to 7, each once
Outputs:
- quant_out: bfloat16 [5120, 32768], P(None, 'mp')
- scale_out: bfloat16 [5120, 256], P(None, 'mp')
- checksum: float32 [256], replicated
The draws below stay inside these ranges and needn't reach their ends.
Inputs may be any that keep to these rules, and one draw needn't show every extreme that they name: `rank_map`: a permutation of 0 to 7.
All inputs are finite; a program needn't handle non-finite values.
Results may differ from the reference program's by a relative error of at most 0.0085.
Values may be sent and summed in bfloat16 or wider, within the bound.
A program may use at most 192 MiB of HBM per device.

```python
import math
import jax
import jax.numpy as jnp
from jax import lax

D = 5120
F = 32768
N_MP = 8


def level_of(key, shape, pieces, smallest, largest):
    factor_of = 1.0
    for position, parts in pieces:
        draws = jax.random.uniform(jax.random.fold_in(jax.random.fold_in(key, 6), position), (parts,), jnp.float32, smallest / len(pieces), largest / len(pieces))
        factor_of = factor_of * jnp.repeat(jnp.exp(draws), shape[position] // parts).reshape((-1,) + (1,) * (len(shape) - 1 - position))
    return factor_of


def scatter_about(stream_key, dims, deviation, limit, shards=(), dtype=jnp.bfloat16):
    values = jax.random.normal(stream_key, dims, jnp.float32) * deviation
    if len(shards) > 0:
        values = level_of(stream_key, dims, shards, -0.22, 0.18) * values
    return jnp.clip(values, min=-limit, max=limit).astype(dtype)


def setup_inputs(seed: int = 0) -> dict:
    key_of = jax.random.split(jax.random.key(seed), 3)
    weight = scatter_about(key_of[0], (D, F), D ** -0.5, 0.078125, ((0, 4), (1, 8)))
    rank_map = jax.random.permutation(key_of[1], N_MP).astype(jnp.int32)
    return {"weight": weight, "rank_map": rank_map}


floor_ratio = 0.25

def quantize(weight):
    rows, cols = weight.shape
    blocks = weight.astype(jnp.float32).reshape(rows, cols // 128, 128)
    peak = lax.optimization_barrier(jnp.max(jnp.abs(blocks), axis=2))
    scale = (jnp.maximum(peak, floor_ratio / math.sqrt(D)) / 127.0).astype(jnp.bfloat16)
    quant = (blocks / scale.astype(jnp.float32)[:, :, None]).astype(jnp.bfloat16)
    return (quant, scale)

def inverse(rank_map):
    count = rank_map.shape[0]
    ids = jnp.arange(count).astype(jnp.int32)
    match = (rank_map[None, :] == ids[:, None]).astype(jnp.int32)
    return lax.optimization_barrier(jnp.sum(ids[None, :] * match, axis=1)).astype(jnp.int32)

def reference(weight, rank_map):
    quant, scale = quantize(weight)
    total = lax.optimization_barrier(jnp.sum(quant.astype(jnp.float32), axis=(0, 2)))
    checksum = total / (127.0 * math.sqrt(D * 128))
    inv = inverse(rank_map)
    blocks = F // 128
    local = blocks // N_MP
    order = (jnp.arange(local).astype(jnp.int32)[None, :] * N_MP + inv[:, None]).reshape(-1).astype(jnp.int32)
    quant_out = jnp.take(quant, order, axis=1).reshape(D, F)
    scale_out = jnp.take(scale, order, axis=1)
    return (quant_out, scale_out, checksum)
```

```python
import functools
import math

import jax
import jax.numpy as jnp
from jax import lax
from jax.experimental import pallas as pl
from jax.experimental.pallas import tpu as pltpu
from jax.sharding import PartitionSpec as P


LANES = 128
FLOOR_RATIO = 0.25
MESH = pl.DeviceIdType.MESH
GRAIN = 32
VMEM_LIMIT = 57 * 1024 * 1024
FILL_LIMIT = 8 * 1024 * 1024


def flip(m, k):
    bit, out = 1, m
    while bit <= k:
        if k & bit:
            out = out + bit - 2 * bit * ((m // bit) % 2)
        bit *= 2
    return out


def scales_of(blocks, height, floor):
    lane = lax.broadcasted_iota(jnp.int32, (height, LANES), 1)
    peaks = jnp.zeros((height, LANES), jnp.float32)
    for b, read in enumerate(blocks):
        peak = jnp.max(jnp.abs(read().astype(jnp.float32)), axis=1, keepdims=True)
        peaks = jnp.where(lane == b, peak, peaks)
    return (jnp.maximum(peaks, floor) / 127.0).astype(jnp.bfloat16).astype(jnp.float32)


def quantize_rows(x_ref, rows, floor):
    nblocks = x_ref.shape[1] // LANES
    blocks = [lambda b=b: x_ref[rows, b * LANES:(b + 1) * LANES] for b in range(nblocks)]
    scale = scales_of(blocks, GRAIN, floor)
    inverse = 1.0 / scale
    yield scale
    for b, read in enumerate(blocks):
        yield (read().astype(jnp.float32) * inverse[:, b:b + 1]).astype(jnp.bfloat16)


def quantize_tile(floor, x_ref, q_ref, s_ref, scales):
    @pl.loop(0, LANES // GRAIN)
    def _(t):
        rows = pl.ds(pl.multiple_of(t * GRAIN, GRAIN), GRAIN)
        parts = quantize_rows(x_ref, rows, floor)
        scales[rows, :] = next(parts)
        for b, part in enumerate(parts):
            q_ref[rows, b * LANES:(b + 1) * LANES] = part

    s_ref[...] = scales[...].T[:s_ref.shape[0]].astype(jnp.bfloat16)


def quantize_all(landed, floor):
    rows, cols = landed.shape
    nblocks = cols // LANES
    return pl.pallas_call(
        functools.partial(quantize_tile, floor),
        grid=(rows // LANES,),
        in_specs=[pl.BlockSpec((LANES, cols), lambda t: (t, 0))],
        out_specs=[pl.BlockSpec((LANES, cols), lambda t: (t, 0)), pl.BlockSpec((nblocks, LANES), lambda t: (0, t))],
        out_shape=[jax.ShapeDtypeStruct((rows, cols), jnp.bfloat16), jax.ShapeDtypeStruct((nblocks, rows), jnp.bfloat16)],
        scratch_shapes=[pltpu.VMEM((LANES, LANES), jnp.float32)],
        compiler_params=pltpu.CompilerParams(dimension_semantics=("arbitrary",)),
        cost_estimate=pl.CostEstimate(flops=rows * cols * 4, bytes_accessed=rows * cols * 4, transcendentals=0),
    )(landed)


def fill_kernel(n, rows, first, floor, got_ref, _q, _s, q_ref, s_ref, q_v, s_v, scales, sems):
    z = lax.axis_index("dp")

    @pl.when(jnp.logical_or(z == 0, z == n - 1))
    def _():
        quantize_tile(floor, got_ref, q_v, s_v, scales)
        place = pl.ds(pl.multiple_of(jnp.where(z == 0, 1, n - 2) * rows + first, LANES), LANES)
        copies = [pltpu.make_async_copy(q_v, q_ref.at[place], sems.at[0]),
                  pltpu.make_async_copy(s_v, s_ref.at[:, place], sems.at[1])]
        for copy in copies:
            copy.start()
        for copy in copies:
            copy.wait()


def fill(quant, scale, got, n, rows, first, floor):
    size, cols = got.shape
    any_spec = pl.BlockSpec(memory_space=pl.ANY)
    return pl.pallas_call(
        functools.partial(fill_kernel, n, rows, first, floor),
        in_specs=[pl.BlockSpec(memory_space=pltpu.VMEM), any_spec, any_spec],
        out_specs=[any_spec] * 2,
        out_shape=[jax.ShapeDtypeStruct(quant.shape, quant.dtype), jax.ShapeDtypeStruct(scale.shape, scale.dtype)],
        input_output_aliases={1: 0, 2: 1},
        scratch_shapes=[
            pltpu.VMEM((size, cols), quant.dtype),
            pltpu.VMEM((scale.shape[0], LANES), scale.dtype),
            pltpu.VMEM((LANES, LANES), jnp.float32),
            pltpu.SemaphoreType.DMA((2,)),
        ],
        compiler_params=pltpu.CompilerParams(vmem_limit_bytes=FILL_LIMIT),
        cost_estimate=pl.CostEstimate(flops=size * cols * 4, bytes_accessed=size * cols * 4, transcendentals=0),
    )(got, quant, scale)


def move_kernel(n, count, spans, floor, map_ref, w_ref, out_ref, tail_ref, last_ref, sum_ref,
                stage, perm, acc, zsum, total, psum,
                load_sem, own_sem, tail_sem, a_send, a_recv, z_send, z_recv):
    z = lax.axis_index("dp")
    m = lax.axis_index("mp")
    rows, width = perm.shape[1:]
    group = width // LANES
    nblocks = count * group
    chunks = len(spans)
    TAIL, SUM = chunks - 1, chunks
    order = sorted(range(1, count), key=lambda k: (bin(k).count("1"), k))

    def when(cond, act):
        @pl.when(cond)
        def _():
            act()

    loads = [pltpu.make_async_copy(w_ref.at[pl.ds(*span)], stage.at[pl.ds(*span)], load_sem.at[c])
             for c, span in enumerate(spans)]
    for load in loads:
        load.start()

    barrier = pltpu.get_barrier_semaphore()
    for k in range(1, count):
        pl.semaphore_signal(barrier, inc=1, device_id=(z, flip(m, k)), device_id_type=MESH)
    when(z > 0, lambda: pl.semaphore_signal(barrier, inc=1, device_id=(z - 1, m), device_id_type=MESH))
    when(z < n - 1, lambda: pl.semaphore_signal(barrier, inc=1, device_id=(z + 1, m), device_id_type=MESH))
    beside = jnp.where(z > 0, 1, 0) + jnp.where(z < n - 1, 1, 0)

    holds = [[map_ref[j] == r for j in range(count)] for r in range(count)]

    def arrange(c):
        start, size = spans[c]
        loads[c].wait()

        @pl.loop(0, size // GRAIN)
        def _(t):
            here = pl.ds(pl.multiple_of(start + t * GRAIN, GRAIN), GRAIN)
            for i in range(group):
                first = i * count
                blocks = [stage[here, (first + j) * LANES:(first + j + 1) * LANES] for j in range(count)]
                for r in range(count):
                    block = blocks[0]
                    for j in range(1, count):
                        block = jnp.where(holds[r][j], blocks[j], block)
                    perm[r, here, i * LANES:(i + 1) * LANES] = block

    def place(origin, c, src):
        start, size = spans[c]
        return out_ref.at[pl.ds(pl.multiple_of(origin * rows + start, 16), size),
                          pl.ds(pl.multiple_of(src * width, LANES), width)]

    def own(c):
        return perm.at[m, pl.ds(*spans[c])]

    def plane(c, k):
        peer = flip(m, k)
        if c == SUM:
            src, dst = total, psum.at[m]
        else:
            src, dst = perm.at[peer, pl.ds(*spans[c])], place(z, c, m)
        return pltpu.make_async_remote_copy(
            src_ref=src, dst_ref=dst, send_sem=a_send.at[c, k - 1], recv_sem=a_recv.at[c, k - 1],
            device_id=(z, peer), device_id_type=MESH)

    def ring(unit, way, hop):
        c, k = unit
        origin = z - way * (hop - 1)
        if c == SUM:
            src = dst = zsum.at[origin]
        else:
            dst = place(origin, c, flip(m, k))
            src = own(c) if hop == 1 and k == 0 else dst
        w = 0 if way == 1 else 1
        return pltpu.make_async_remote_copy(
            src_ref=src, dst_ref=dst, send_sem=z_send.at[w, hop - 1, c, k], recv_sem=z_recv.at[w, hop - 1, c, k],
            device_id=(z + way, m), device_id_type=MESH)

    def sends(unit, way, hop):
        later = hop == 1 and unit[0] == TAIL
        if way == -1:
            return jnp.logical_and(z > (1 if later else 0), z + hop - 1 <= n - 1)
        return jnp.logical_and(z < n - (2 if later else 1), z - (hop - 1) >= 0)

    def gets(unit, way, hop):
        later = hop == 1 and unit[0] == TAIL
        if way == -1:
            return jnp.logical_and(z >= (1 if later else 0), z + hop <= n - 1)
        return jnp.logical_and(z <= n - (2 if later else 1), z - hop >= 0)

    def start_ring(unit):
        for way in (-1, 1):
            when(sends(unit, way, 1), lambda way=way: ring(unit, way, 1).start())

    def keep(c):
        return pltpu.make_async_copy(own(c), place(z, c, m), own_sem.at[c])

    def send_own(c):
        start_ring((c, 0))
        for k in order:
            plane(c, k).start()
        keep(c).start()

    def add_up(first, size):
        @pl.loop(0, size // GRAIN)
        def _(t):
            parts = quantize_rows(stage, pl.ds(pl.multiple_of(first + t * GRAIN, GRAIN), GRAIN), floor)
            next(parts)
            for b, part in enumerate(parts):
                acc[b] += jnp.sum(part.astype(jnp.float32).reshape(GRAIN // 8, 8, LANES), axis=0)

    acc[...] = jnp.zeros_like(acc)
    arrange(0)
    pl.semaphore_wait(barrier, count - 1 + beside)
    send_own(0)
    arrange(1)
    for c in range(2, chunks):
        arrange(c)
        send_own(c - 1)
    add_up(*spans[0])
    send_own(TAIL)
    add_up(spans[0][1], rows - spans[0][1])

    sums = jnp.sum(jnp.sum(acc[...], axis=1), axis=1, keepdims=True)
    row = lax.broadcasted_iota(jnp.int32, (nblocks, LANES), 0)
    col = lax.broadcasted_iota(jnp.int32, (nblocks, LANES), 1)
    line = jnp.sum(jnp.where(row == col, sums, 0.0), axis=0, keepdims=True)
    zsum[z] = jnp.broadcast_to(line, zsum.shape[1:])

    blocks = [(c, k) for c in range(chunks) for k in [0] + order]
    for c, k in blocks:
        if k > 0:
            plane(c, k).wait_recv()
            start_ring((c, k))
            if (c, k) == (0, order[-1]):
                start_ring((SUM, 0))

    keep(TAIL).wait()
    start = spans[TAIL][0]
    tail_out = []
    for i, ref in enumerate((tail_ref, last_ref)):
        here = pl.ds(pl.multiple_of(z * rows + start + i * LANES, 16), LANES)
        tail_out.append(pltpu.make_async_copy(out_ref.at[here], ref, tail_sem.at[i]))
    for copy in tail_out:
        copy.start()

    units = [(SUM, 0)] + blocks
    for hop in range(2, n):
        for unit in units:
            for way in (-1, 1):
                def forward(unit=unit, way=way, hop=hop):
                    ring(unit, way, hop - 1).wait_recv()
                    ring(unit, way, hop).start()

                when(sends(unit, way, hop), forward)

    def settle(unit, way, hop):
        stays = z == 0 if way == -1 else z == n - 1
        when(jnp.logical_and(gets(unit, way, hop), stays), lambda: ring(unit, way, hop).wait_recv())

    for hop in range(1, n):
        for way in (-1, 1):
            settle((SUM, 0), way, hop)
    whole = zsum[0]
    for origin in range(1, n):
        whole = whole + zsum[origin]
    total[...] = whole
    psum[m] = whole
    for copy in tail_out:
        copy.wait()
    for c in range(chunks):
        if c != TAIL:
            keep(c).wait()
        for k in order:
            plane(c, k).wait_send()
    for k in order:
        plane(SUM, k).start()
    for k in order:
        plane(SUM, k).wait()
    sum_ref[...] = psum[...]

    for hop in range(1, n):
        for unit in units:
            for way in (-1, 1):
                if unit[0] != SUM:
                    settle(unit, way, hop)
                when(sends(unit, way, hop),
                     lambda unit=unit, way=way, hop=hop: ring(unit, way, hop).wait_send())


def move(weight, rank_map, n, spans, floor):
    rows, cols = weight.shape
    count = rank_map.shape[0]
    width = cols // count
    nblocks = cols // LANES
    chunks = len(spans)
    any_spec = pl.BlockSpec(memory_space=pl.ANY)
    dma = pltpu.SemaphoreType.DMA
    sent = rows * cols * 2 * (n - 1)
    return pl.pallas_call(
        functools.partial(move_kernel, n, count, spans, floor),
        in_specs=[pl.BlockSpec(memory_space=pltpu.SMEM), any_spec],
        out_specs=[any_spec] + [pl.BlockSpec(memory_space=pltpu.VMEM)] * 3,
        out_shape=[
            jax.ShapeDtypeStruct((n * rows, cols), weight.dtype),
            jax.ShapeDtypeStruct((LANES, cols), weight.dtype),
            jax.ShapeDtypeStruct((LANES, cols), weight.dtype),
            jax.ShapeDtypeStruct((count, 8, LANES), jnp.float32),
        ],
        scratch_shapes=[
            pltpu.VMEM((rows, cols), weight.dtype),
            pltpu.VMEM((count, rows, width), weight.dtype),
            pltpu.VMEM((nblocks, 8, LANES), jnp.float32),
            pltpu.VMEM((n, 8, LANES), jnp.float32),
            pltpu.VMEM((8, LANES), jnp.float32),
            pltpu.VMEM((count, 8, LANES), jnp.float32),
            dma((chunks,)),
            dma((chunks,)),
            dma((2,)),
            dma((chunks + 1, count - 1)),
            dma((chunks + 1, count - 1)),
            dma((2, n - 1, chunks + 1, count)),
            dma((2, n - 1, chunks + 1, count)),
        ],
        compiler_params=pltpu.CompilerParams(collective_id=0, has_side_effects=True, vmem_limit_bytes=VMEM_LIMIT),
        cost_estimate=pl.CostEstimate(flops=rows * cols * 8, bytes_accessed=sent * 2, transcendentals=0),
    )(rank_map, weight)


def local(n, weight, rank_map):
    rows, cols = weight.shape
    nblocks = cols // LANES
    total_rows = rows * n
    floor = FLOOR_RATIO / math.sqrt(total_rows)
    main = rows - 2 * LANES
    rest = (main - LANES) // 2
    spans = ((0, LANES), (LANES, rest), (LANES + rest, rest), (main, 2 * LANES))
    ends = [(1, 0), (n - 2, n - 1)]

    landed, tail_own, last_own, sums = move(weight, rank_map, n, spans, floor)
    tail_got = lax.ppermute(tail_own, "dp", ends)
    last_got = lax.ppermute(last_own, "dp", ends)
    quant, scale = quantize_all(landed, floor)
    quant, scale = fill(quant, scale, tail_got, n, rows, main, floor)
    quant, scale = fill(quant, scale, last_got, n, rows, main + LANES, floor)
    totals = sums[:, 0, :nblocks].reshape(-1)
    return (quant, scale.T, totals / (127.0 * math.sqrt(total_rows * LANES)))


def solution(mesh):
    n = mesh.shape["dp"]
    in_specs = (P("dp", "mp"), P())
    out_specs = (P(None, "mp"), P(None, "mp"), P())

    def body(weight, rank_map):
        return local(n, weight, rank_map)

    return jax.shard_map(body, mesh=mesh, in_specs=in_specs, out_specs=out_specs, check_vma=False)
```

```python
import functools
import math

import jax
import jax.numpy as jnp
from jax import lax
from jax.experimental import pallas as pl
from jax.experimental.pallas import tpu as pltpu
from jax.sharding import PartitionSpec as P


LANES = 128
FLOOR_RATIO = 0.25
MESH = pl.DeviceIdType.MESH
GRAIN = 32
TILE = 2 * LANES
VMEM_LIMIT = 57 * 1024 * 1024
FILL_LIMIT = 8 * 1024 * 1024


def flip(m, k):
    bit, out = 1, m
    while bit <= k:
        if k & bit:
            out = out + bit - 2 * bit * ((m // bit) % 2)
        bit *= 2
    return out


def write_spread(spread, nblocks):
    lane = lax.broadcasted_iota(jnp.int32, (LANES, LANES), 0)
    for b in range(nblocks):
        hit = jnp.logical_and(lax.rem(lane, nblocks) == b, lane < 3 * nblocks)
        spread[:, b * LANES:(b + 1) * LANES] = jnp.where(hit, 1.0, 0.0).astype(jnp.bfloat16)


def quantize_rows(x_ref, rows, spread, floor):
    nblocks = x_ref.shape[1] // LANES
    shape = (LANES, LANES)
    lane = lax.broadcasted_iota(jnp.int32, shape, 1)
    slot = lax.rem(lane, nblocks)
    peaks = jnp.zeros(shape, jnp.bfloat16)
    for b in range(nblocks):
        peak = jnp.max(jnp.abs(x_ref[rows, b * LANES:(b + 1) * LANES]), axis=1, keepdims=True)
        peaks = jnp.where(slot == b, peak, peaks)
    scale = (jnp.maximum(peaks.astype(jnp.float32), floor) / 127.0).astype(jnp.bfloat16).astype(jnp.float32)
    yield scale
    inverse = 1.0 / scale
    high = inverse.astype(jnp.bfloat16).astype(jnp.float32)
    middle = (inverse - high).astype(jnp.bfloat16).astype(jnp.float32)
    low = inverse - high - middle
    parts = jnp.where(lane < nblocks, high, jnp.where(lane < 2 * nblocks, middle, low)).astype(jnp.bfloat16)
    for b in range(0, nblocks, 2):
        factor = jnp.dot(parts, spread[:, b * LANES:(b + 2) * LANES], preferred_element_type=jnp.float32)
        pair = x_ref[rows, b * LANES:(b + 2) * LANES].astype(jnp.float32) * factor
        for i in range(2):
            yield pair[:, i * LANES:(i + 1) * LANES].astype(jnp.bfloat16)


def quantize_tile(floor, x_ref, q_ref, s_ref, spread):
    @pl.loop(0, x_ref.shape[0] // LANES)
    def _(t):
        rows = pl.ds(pl.multiple_of(t * LANES, LANES), LANES)
        parts = quantize_rows(x_ref, rows, spread, floor)
        s_ref[:, rows] = next(parts).T[:s_ref.shape[0]].astype(jnp.bfloat16)
        for b, part in enumerate(parts):
            q_ref[rows, b * LANES:(b + 1) * LANES] = part


def quantize_kernel(floor, x_ref, q_ref, s_ref, spread):
    @pl.when(pl.program_id(0) == 0)
    def _():
        write_spread(spread, s_ref.shape[0])

    quantize_tile(floor, x_ref, q_ref, s_ref, spread)


def quantize_all(landed, floor):
    rows, cols = landed.shape
    nblocks = cols // LANES
    tile = TILE
    return pl.pallas_call(
        functools.partial(quantize_kernel, floor),
        grid=(rows // tile,),
        in_specs=[pl.BlockSpec((tile, cols), lambda t: (t, 0))],
        out_specs=[pl.BlockSpec((tile, cols), lambda t: (t, 0)), pl.BlockSpec((nblocks, tile), lambda t: (0, t))],
        out_shape=[jax.ShapeDtypeStruct((rows, cols), jnp.bfloat16), jax.ShapeDtypeStruct((nblocks, rows), jnp.bfloat16)],
        scratch_shapes=[pltpu.VMEM((LANES, cols), jnp.bfloat16)],
        compiler_params=pltpu.CompilerParams(dimension_semantics=("arbitrary",)),
        cost_estimate=pl.CostEstimate(flops=rows * cols * 4, bytes_accessed=rows * cols * 4, transcendentals=0),
    )(landed)


def fill_kernel(n, rows, first, floor, got_ref, _q, _s, q_ref, s_ref, q_v, s_v, spread, sems):
    z = lax.axis_index("dp")

    @pl.when(jnp.logical_or(z == 0, z == n - 1))
    def _():
        write_spread(spread, s_v.shape[0])
        quantize_tile(floor, got_ref, q_v, s_v, spread)
        place = pl.ds(pl.multiple_of(jnp.where(z == 0, 1, n - 2) * rows + first, LANES), q_v.shape[0])
        copies = [pltpu.make_async_copy(q_v, q_ref.at[place], sems.at[0]),
                  pltpu.make_async_copy(s_v, s_ref.at[:, place], sems.at[1])]
        for copy in copies:
            copy.start()
        for copy in copies:
            copy.wait()


def fill(quant, scale, got, n, rows, first, floor):
    size, cols = got.shape
    any_spec = pl.BlockSpec(memory_space=pl.ANY)
    return pl.pallas_call(
        functools.partial(fill_kernel, n, rows, first, floor),
        in_specs=[pl.BlockSpec(memory_space=pltpu.VMEM), any_spec, any_spec],
        out_specs=[any_spec] * 2,
        out_shape=[jax.ShapeDtypeStruct(quant.shape, quant.dtype), jax.ShapeDtypeStruct(scale.shape, scale.dtype)],
        input_output_aliases={1: 0, 2: 1},
        scratch_shapes=[
            pltpu.VMEM((size, cols), quant.dtype),
            pltpu.VMEM((scale.shape[0], size), scale.dtype),
            pltpu.VMEM((LANES, cols), jnp.bfloat16),
            pltpu.SemaphoreType.DMA((2,)),
        ],
        compiler_params=pltpu.CompilerParams(vmem_limit_bytes=FILL_LIMIT),
        cost_estimate=pl.CostEstimate(flops=size * cols * 4, bytes_accessed=size * cols * 4, transcendentals=0),
    )(got, quant, scale)


def move_kernel(n, count, spans, floor, map_ref, w_ref, out_ref, tail_ref, last_ref, sum_ref,
                stage, perm, spread, acc, zsum, total, psum,
                load_sem, own_sem, tail_sem, a_send, a_recv, z_send, z_recv):
    z = lax.axis_index("dp")
    m = lax.axis_index("mp")
    rows, width = perm.shape[1:]
    group = width // LANES
    nblocks = count * group
    chunks = len(spans)
    TAIL, SUM = chunks - 1, chunks
    order = sorted(range(1, count), key=lambda k: (bin(k).count("1"), k))

    def when(cond, act):
        @pl.when(cond)
        def _():
            act()

    loads = [pltpu.make_async_copy(w_ref.at[pl.ds(*span)], stage.at[pl.ds(*span)], load_sem.at[c])
             for c, span in enumerate(spans)]
    for load in loads:
        load.start()

    barrier = pltpu.get_barrier_semaphore()
    for k in range(1, count):
        pl.semaphore_signal(barrier, inc=1, device_id=(z, flip(m, k)), device_id_type=MESH)
    when(z > 0, lambda: pl.semaphore_signal(barrier, inc=1, device_id=(z - 1, m), device_id_type=MESH))
    when(z < n - 1, lambda: pl.semaphore_signal(barrier, inc=1, device_id=(z + 1, m), device_id_type=MESH))
    beside = jnp.where(z > 0, 1, 0) + jnp.where(z < n - 1, 1, 0)

    holds = [[map_ref[j] == r for j in range(count)] for r in range(count)]

    def arrange(c):
        start, size = spans[c]
        loads[c].wait()

        @pl.loop(0, size // GRAIN)
        def _(t):
            here = pl.ds(pl.multiple_of(start + t * GRAIN, GRAIN), GRAIN)
            for i in range(group):
                first = i * count
                blocks = [stage[here, (first + j) * LANES:(first + j + 1) * LANES] for j in range(count)]
                for r in range(count):
                    block = blocks[0]
                    for j in range(1, count):
                        block = jnp.where(holds[r][j], blocks[j], block)
                    perm[r, here, i * LANES:(i + 1) * LANES] = block

    def place(origin, c, src):
        start, size = spans[c]
        return out_ref.at[pl.ds(pl.multiple_of(origin * rows + start, 16), size),
                          pl.ds(pl.multiple_of(src * width, LANES), width)]

    def own(c):
        return perm.at[m, pl.ds(*spans[c])]

    def plane(c, k):
        peer = flip(m, k)
        if c == SUM:
            src, dst = total, psum.at[m]
        else:
            src, dst = perm.at[peer, pl.ds(*spans[c])], place(z, c, m)
        return pltpu.make_async_remote_copy(
            src_ref=src, dst_ref=dst, send_sem=a_send.at[c, k - 1], recv_sem=a_recv.at[c, k - 1],
            device_id=(z, peer), device_id_type=MESH)

    def ring(unit, way, hop):
        c, k = unit
        origin = z - way * (hop - 1)
        if c == SUM:
            src = dst = zsum.at[origin]
        else:
            dst = place(origin, c, flip(m, k))
            src = own(c) if hop == 1 and k == 0 else dst
        w = 0 if way == 1 else 1
        return pltpu.make_async_remote_copy(
            src_ref=src, dst_ref=dst, send_sem=z_send.at[w, hop - 1, c, k], recv_sem=z_recv.at[w, hop - 1, c, k],
            device_id=(z + way, m), device_id_type=MESH)

    def sends(unit, way, hop):
        later = hop == 1 and unit[0] == TAIL
        if way == -1:
            return jnp.logical_and(z > (1 if later else 0), z + hop - 1 <= n - 1)
        return jnp.logical_and(z < n - (2 if later else 1), z - (hop - 1) >= 0)

    def gets(unit, way, hop):
        later = hop == 1 and unit[0] == TAIL
        if way == -1:
            return jnp.logical_and(z >= (1 if later else 0), z + hop <= n - 1)
        return jnp.logical_and(z <= n - (2 if later else 1), z - hop >= 0)

    def start_ring(unit):
        for way in (-1, 1):
            when(sends(unit, way, 1), lambda way=way: ring(unit, way, 1).start())

    def keep(c):
        return pltpu.make_async_copy(own(c), place(z, c, m), own_sem.at[c])

    def send_own(c):
        start_ring((c, 0))
        for k in order:
            plane(c, k).start()
        keep(c).start()

    def add_up(first, size):
        @pl.loop(0, size // LANES)
        def _(t):
            parts = quantize_rows(stage, pl.ds(pl.multiple_of(first + t * LANES, LANES), LANES), spread, floor)
            next(parts)
            for b, part in enumerate(parts):
                acc[b] += jnp.sum(part.astype(jnp.float32).reshape(LANES // 8, 8, LANES), axis=0)

    arrange(0)
    pl.semaphore_wait(barrier, count - 1 + beside)
    send_own(0)
    arrange(1)
    for c in range(2, chunks):
        arrange(c)
        send_own(c - 1)
    acc[...] = jnp.zeros_like(acc)
    write_spread(spread, nblocks)
    add_up(*spans[0])
    send_own(TAIL)
    add_up(spans[0][1], rows - spans[0][1])

    sums = jnp.sum(jnp.sum(acc[...], axis=1), axis=1, keepdims=True)
    row = lax.broadcasted_iota(jnp.int32, (nblocks, LANES), 0)
    col = lax.broadcasted_iota(jnp.int32, (nblocks, LANES), 1)
    line = jnp.sum(jnp.where(row == col, sums, 0.0), axis=0, keepdims=True)
    zsum[z] = jnp.broadcast_to(line, zsum.shape[1:])

    blocks = [(c, k) for c in range(chunks) for k in [0] + order]
    for c, k in blocks:
        if k > 0:
            plane(c, k).wait_recv()
            start_ring((c, k))
            if (c, k) == (0, order[-1]):
                start_ring((SUM, 0))

    keep(TAIL).wait()
    start = spans[TAIL][0]
    tail_out = []
    for i, ref in enumerate((tail_ref, last_ref)):
        here = pl.ds(pl.multiple_of(z * rows + start + i * LANES, 16), LANES)
        tail_out.append(pltpu.make_async_copy(out_ref.at[here], ref, tail_sem.at[i]))
    for copy in tail_out:
        copy.start()

    units = [(SUM, 0)] + blocks
    for hop in range(2, n):
        for unit in units:
            for way in (-1, 1):
                def forward(unit=unit, way=way, hop=hop):
                    ring(unit, way, hop - 1).wait_recv()
                    ring(unit, way, hop).start()

                when(sends(unit, way, hop), forward)

    def settle(unit, way, hop):
        stays = z == 0 if way == -1 else z == n - 1
        when(jnp.logical_and(gets(unit, way, hop), stays), lambda: ring(unit, way, hop).wait_recv())

    for hop in range(1, n):
        for way in (-1, 1):
            settle((SUM, 0), way, hop)
    whole = zsum[0]
    for origin in range(1, n):
        whole = whole + zsum[origin]
    total[...] = whole
    psum[m] = whole
    for copy in tail_out:
        copy.wait()
    for c in range(chunks):
        if c != TAIL:
            keep(c).wait()
        for k in order:
            plane(c, k).wait_send()
    for k in order:
        plane(SUM, k).start()
    for k in order:
        plane(SUM, k).wait()
    sum_ref[...] = psum[...]

    for hop in range(1, n):
        for unit in units:
            for way in (-1, 1):
                if unit[0] != SUM:
                    settle(unit, way, hop)
                when(sends(unit, way, hop),
                     lambda unit=unit, way=way, hop=hop: ring(unit, way, hop).wait_send())


def move(weight, rank_map, n, spans, floor):
    rows, cols = weight.shape
    count = rank_map.shape[0]
    width = cols // count
    nblocks = cols // LANES
    chunks = len(spans)
    any_spec = pl.BlockSpec(memory_space=pl.ANY)
    dma = pltpu.SemaphoreType.DMA
    sent = rows * cols * 2 * (n - 1)
    return pl.pallas_call(
        functools.partial(move_kernel, n, count, spans, floor),
        in_specs=[pl.BlockSpec(memory_space=pltpu.SMEM), any_spec],
        out_specs=[any_spec] + [pl.BlockSpec(memory_space=pltpu.VMEM)] * 3,
        out_shape=[
            jax.ShapeDtypeStruct((n * rows, cols), weight.dtype),
            jax.ShapeDtypeStruct((LANES, cols), weight.dtype),
            jax.ShapeDtypeStruct((LANES, cols), weight.dtype),
            jax.ShapeDtypeStruct((count, 8, LANES), jnp.float32),
        ],
        scratch_shapes=[
            pltpu.VMEM((rows, cols), weight.dtype),
            pltpu.VMEM((count, rows, width), weight.dtype),
            pltpu.VMEM((LANES, cols), jnp.bfloat16),
            pltpu.VMEM((nblocks, 8, LANES), jnp.float32),
            pltpu.VMEM((n, 8, LANES), jnp.float32),
            pltpu.VMEM((8, LANES), jnp.float32),
            pltpu.VMEM((count, 8, LANES), jnp.float32),
            dma((chunks,)),
            dma((chunks,)),
            dma((2,)),
            dma((chunks + 1, count - 1)),
            dma((chunks + 1, count - 1)),
            dma((2, n - 1, chunks + 1, count)),
            dma((2, n - 1, chunks + 1, count)),
        ],
        compiler_params=pltpu.CompilerParams(collective_id=0, has_side_effects=True, vmem_limit_bytes=VMEM_LIMIT),
        cost_estimate=pl.CostEstimate(flops=rows * cols * 8, bytes_accessed=sent * 2, transcendentals=0),
    )(rank_map, weight)


def local(n, weight, rank_map):
    rows, cols = weight.shape
    nblocks = cols // LANES
    total_rows = rows * n
    floor = FLOOR_RATIO / math.sqrt(total_rows)
    main = rows - 2 * LANES
    rest = (main - LANES) // 2
    spans = ((0, LANES), (LANES, rest), (LANES + rest, rest), (main, 2 * LANES))
    ends = [(1, 0), (n - 2, n - 1)]

    landed, tail_own, last_own, sums = move(weight, rank_map, n, spans, floor)
    tail_got = lax.ppermute(tail_own, "dp", ends)
    last_got = lax.ppermute(last_own, "dp", ends)
    quant, scale = quantize_all(landed, floor)
    quant, scale = fill(quant, scale, tail_got, n, rows, main, floor)
    quant, scale = fill(quant, scale, last_got, n, rows, main + LANES, floor)
    totals = sums[:, 0, :nblocks].reshape(-1)
    return (quant, scale.T, totals / (127.0 * math.sqrt(total_rows * LANES)))


def solution(mesh):
    n = mesh.shape["dp"]
    in_specs = (P("dp", "mp"), P())
    out_specs = (P(None, "mp"), P(None, "mp"), P())

    def body(weight, rank_map):
        return local(n, weight, rank_map)

    return jax.shard_map(body, mesh=mesh, in_specs=in_specs, out_specs=out_specs, check_vma=False)
```

```python
import functools
import math

import jax
import jax.numpy as jnp
from jax import lax
from jax.experimental import pallas as pl
from jax.experimental.pallas import tpu as pltpu
from jax.sharding import PartitionSpec as P


LANES = 128
FLOOR_RATIO = 0.25
MESH = pl.DeviceIdType.MESH
GRAIN = 32
TILE = 4 * LANES
VMEM_LIMIT = 57 * 1024 * 1024
QUANT_LIMIT = 40 * 1024 * 1024
FILL_LIMIT = 8 * 1024 * 1024


def flip(m, k):
    bit, out = 1, m
    while bit <= k:
        if k & bit:
            out = out + bit - 2 * bit * ((m // bit) % 2)
        bit *= 2
    return out


def write_spread(spread, nblocks):
    lane = lax.broadcasted_iota(jnp.int32, (LANES, LANES), 0)
    for b in range(nblocks):
        hit = jnp.logical_and(lax.rem(lane, nblocks) == b, lane < 3 * nblocks)
        spread[:, b * LANES:(b + 1) * LANES] = jnp.where(hit, 1.0, 0.0).astype(jnp.bfloat16)


def quantize_rows(x_ref, rows, spread, floor):
    nblocks = x_ref.shape[1] // LANES
    shape = (LANES, LANES)
    lane = lax.broadcasted_iota(jnp.int32, shape, 1)
    slot = lax.rem(lane, nblocks)
    peaks = jnp.zeros(shape, jnp.float32)
    for b in range(nblocks):
        peak = jnp.max(jnp.abs(x_ref[rows, b * LANES:(b + 1) * LANES]), axis=1, keepdims=True)
        peaks = jnp.where(slot == b, peak.astype(jnp.float32), peaks)
    scale = (jnp.maximum(peaks, floor) / 127.0).astype(jnp.bfloat16).astype(jnp.float32)
    yield scale
    inverse = 1.0 / scale
    high = inverse.astype(jnp.bfloat16).astype(jnp.float32)
    middle = (inverse - high).astype(jnp.bfloat16).astype(jnp.float32)
    low = inverse - high - middle
    parts = jnp.where(lane < nblocks, high, jnp.where(lane < 2 * nblocks, middle, low)).astype(jnp.bfloat16)
    for b in range(0, nblocks, 2):
        factor = jnp.dot(parts, spread[:, b * LANES:(b + 2) * LANES], preferred_element_type=jnp.float32)
        pair = x_ref[rows, b * LANES:(b + 2) * LANES].astype(jnp.float32) * factor
        yield pair.astype(jnp.bfloat16)


def quantize_tile(floor, x_ref, q_ref, s_ref, spread):
    tiles = x_ref.shape[0] // LANES

    @pl.loop(0, tiles, unroll=tiles)
    def _(t):
        rows = pl.ds(pl.multiple_of(t * LANES, LANES), LANES)
        parts = quantize_rows(x_ref, rows, spread, floor)
        s_ref[:, rows] = next(parts).T[:s_ref.shape[0]].astype(jnp.bfloat16)
        for b, part in enumerate(parts):
            q_ref[rows, b * 2 * LANES:(b + 1) * 2 * LANES] = part


def quantize_kernel(floor, x_ref, q_ref, s_ref, spread):
    @pl.when(pl.program_id(0) == 0)
    def _():
        write_spread(spread, s_ref.shape[0])

    quantize_tile(floor, x_ref, q_ref, s_ref, spread)


def quantize_all(landed, floor):
    rows, cols = landed.shape
    nblocks = cols // LANES
    tile = TILE
    return pl.pallas_call(
        functools.partial(quantize_kernel, floor),
        grid=(rows // tile,),
        in_specs=[pl.BlockSpec((tile, cols), lambda t: (t, 0))],
        out_specs=[pl.BlockSpec((tile, cols), lambda t: (t, 0)), pl.BlockSpec((nblocks, tile), lambda t: (0, t))],
        out_shape=[jax.ShapeDtypeStruct((rows, cols), jnp.bfloat16), jax.ShapeDtypeStruct((nblocks, rows), jnp.bfloat16)],
        scratch_shapes=[pltpu.VMEM((LANES, cols), jnp.bfloat16)],
        compiler_params=pltpu.CompilerParams(dimension_semantics=("arbitrary",), vmem_limit_bytes=QUANT_LIMIT),
        cost_estimate=pl.CostEstimate(flops=rows * cols * 4, bytes_accessed=rows * cols * 4, transcendentals=0),
    )(landed)


def fill_kernel(n, rows, first, even, floor, got_ref, _q, _s, q_ref, s_ref, q_v, s_v, spread, sems):
    z = lax.axis_index("dp")

    end = jnp.logical_or(z == 0, z == n - 1)
    if even:
        end = jnp.logical_and(end, lax.axis_index("mp") % 2 == 0)

    @pl.when(end)
    def _():
        write_spread(spread, s_v.shape[0])
        quantize_tile(floor, got_ref, q_v, s_v, spread)
        place = pl.ds(pl.multiple_of(jnp.where(z == 0, 1, n - 2) * rows + first, LANES), q_v.shape[0])
        copies = [pltpu.make_async_copy(q_v, q_ref.at[place], sems.at[0]),
                  pltpu.make_async_copy(s_v, s_ref.at[:, place], sems.at[1])]
        for copy in copies:
            copy.start()
        for copy in copies:
            copy.wait()


def fill(quant, scale, got, n, rows, first, even, floor):
    size, cols = got.shape
    any_spec = pl.BlockSpec(memory_space=pl.ANY)
    return pl.pallas_call(
        functools.partial(fill_kernel, n, rows, first, even, floor),
        in_specs=[pl.BlockSpec(memory_space=pltpu.VMEM), any_spec, any_spec],
        out_specs=[any_spec] * 2,
        out_shape=[jax.ShapeDtypeStruct(quant.shape, quant.dtype), jax.ShapeDtypeStruct(scale.shape, scale.dtype)],
        input_output_aliases={1: 0, 2: 1},
        scratch_shapes=[
            pltpu.VMEM((size, cols), quant.dtype),
            pltpu.VMEM((scale.shape[0], size), scale.dtype),
            pltpu.VMEM((LANES, cols), jnp.bfloat16),
            pltpu.SemaphoreType.DMA((2,)),
        ],
        compiler_params=pltpu.CompilerParams(vmem_limit_bytes=FILL_LIMIT),
        cost_estimate=pl.CostEstimate(flops=size * cols * 4, bytes_accessed=size * cols * 4, transcendentals=0),
    )(got, quant, scale)


def move_kernel(n, count, spans, floor, map_ref, w_ref, out_ref, odd_ref, tail_ref, last_ref, sum_ref,
                stage, perm, spread, acc, zsum, total, psum,
                load_sem, own_sem, tail_sem, a_send, a_recv, z_send, z_recv):
    z = lax.axis_index("dp")
    m = lax.axis_index("mp")
    rows, width = perm.shape[1:]
    group = width // LANES
    nblocks = count * group
    MAIN, ODD, TAIL, HEAD, BODY, SUM = range(6)
    order = sorted(range(1, count), key=lambda k: (bin(k).count("1"), k))

    def when(cond, act):
        @pl.when(cond)
        def _():
            act()

    loads = {c: pltpu.make_async_copy(w_ref.at[pl.ds(*spans[c])], stage.at[pl.ds(*spans[c])], load_sem.at[c])
             for c in (HEAD, BODY, ODD, TAIL)}
    for load in loads.values():
        load.start()

    barrier = pltpu.get_barrier_semaphore()
    for k in range(1, count):
        pl.semaphore_signal(barrier, inc=1, device_id=(z, flip(m, k)), device_id_type=MESH)
    when(z > 0, lambda: pl.semaphore_signal(barrier, inc=1, device_id=(z - 1, m), device_id_type=MESH))
    when(z < n - 1, lambda: pl.semaphore_signal(barrier, inc=1, device_id=(z + 1, m), device_id_type=MESH))
    beside = jnp.where(z > 0, 1, 0) + jnp.where(z < n - 1, 1, 0)

    holds = [[map_ref[j] == r for j in range(count)] for r in range(count)]

    def arrange(c):
        start, size = spans[c]
        loads[c].wait()

        @pl.loop(0, size // GRAIN)
        def _(t):
            here = pl.ds(pl.multiple_of(start + t * GRAIN, GRAIN), GRAIN)
            for i in range(group):
                first = i * count
                blocks = [stage[here, (first + j) * LANES:(first + j + 1) * LANES] for j in range(count)]
                for r in range(count):
                    block = blocks[0]
                    for j in range(1, count):
                        block = jnp.where(holds[r][j], blocks[j], block)
                    perm[r, here, i * LANES:(i + 1) * LANES] = block

    def place(origin, c, src):
        start, size = spans[c]
        return out_ref.at[pl.ds(pl.multiple_of(origin * rows + start, 16), size),
                          pl.ds(pl.multiple_of(src * width, LANES), width)]

    def own(c):
        return perm.at[m, pl.ds(*spans[c])]

    def plane(c, k):
        peer = flip(m, k)
        if c == SUM:
            src, dst = total, psum.at[m]
        else:
            src, dst = perm.at[peer, pl.ds(*spans[c])], place(z, c, m)
        return pltpu.make_async_remote_copy(
            src_ref=src, dst_ref=dst, send_sem=a_send.at[c, k - 1], recv_sem=a_recv.at[c, k - 1],
            device_id=(z, peer), device_id_type=MESH)

    def ring(unit, way, hop):
        c, k = unit
        origin = z - way * (hop - 1)
        if c == SUM:
            src = dst = zsum.at[origin]
        else:
            dst = place(origin, c, flip(m, k))
            src = own(c) if hop == 1 and k == 0 else dst
        w = 0 if way == 1 else 1
        return pltpu.make_async_remote_copy(
            src_ref=src, dst_ref=dst, send_sem=z_send.at[w, hop - 1, c, k], recv_sem=z_recv.at[w, hop - 1, c, k],
            device_id=(z + way, m), device_id_type=MESH)

    def kept(unit, hop):
        return {TAIL: 1, ODD: 1 - m % 2}.get(unit[0], 0) if hop == 1 else 0

    def sends(unit, way, hop):
        low = kept(unit, hop)
        if way == -1:
            return jnp.logical_and(z > low, z + hop - 1 <= n - 1)
        return jnp.logical_and(z < n - 1 - low, z - (hop - 1) >= 0)

    def gets(unit, way, hop):
        low = kept(unit, hop)
        if way == -1:
            return jnp.logical_and(z >= low, z + hop <= n - 1)
        return jnp.logical_and(z <= n - 1 - low, z - hop >= 0)

    def start_ring(unit):
        for way in (-1, 1):
            when(sends(unit, way, 1), lambda way=way: ring(unit, way, 1).start())

    def keep(c):
        return pltpu.make_async_copy(own(c), place(z, c, m), own_sem.at[c])

    def send_own(c):
        start_ring((c, 0))
        keep(c).start()

    def send_plane(c):
        for k in order:
            plane(c, k).start()

    def add_up(first, size):
        @pl.loop(0, size // LANES)
        def _(t):
            parts = quantize_rows(stage, pl.ds(pl.multiple_of(first + t * LANES, LANES), LANES), spread, floor)
            next(parts)
            for b, part in enumerate(parts):
                both = part.astype(jnp.float32)
                for i in range(2):
                    one = both[:, i * LANES:(i + 1) * LANES].reshape(LANES // 8, 8, LANES)
                    acc[2 * b + i] += jnp.sum(one, axis=0)

    arrange(HEAD)
    pl.semaphore_wait(barrier, count - 1 + beside)
    send_own(HEAD)
    arrange(BODY)
    send_own(BODY)
    arrange(ODD)
    send_plane(MAIN)
    arrange(TAIL)
    send_own(ODD)
    send_plane(ODD)
    acc[...] = jnp.zeros_like(acc)
    write_spread(spread, nblocks)
    add_up(*spans[HEAD])
    send_own(TAIL)
    send_plane(TAIL)
    add_up(spans[HEAD][1], rows - spans[HEAD][1])

    sums = jnp.sum(jnp.sum(acc[...], axis=1), axis=1, keepdims=True)
    row = lax.broadcasted_iota(jnp.int32, (nblocks, LANES), 0)
    col = lax.broadcasted_iota(jnp.int32, (nblocks, LANES), 1)
    line = jnp.sum(jnp.where(row == col, sums, 0.0), axis=0, keepdims=True)
    zsum[z] = jnp.broadcast_to(line, zsum.shape[1:])

    blocks = [(HEAD, 0), (BODY, 0)] + [(MAIN, k) for k in order] + [(c, k) for c in (ODD, TAIL) for k in [0] + order]
    for c, k in blocks:
        if k > 0:
            plane(c, k).wait_recv()
            start_ring((c, k))
            if (c, k) == (MAIN, order[0]):
                start_ring((SUM, 0))

    keep(ODD).wait()
    keep(TAIL).wait()
    start = spans[ODD][0]
    tail_out = []
    for i, ref in enumerate((odd_ref, tail_ref, last_ref)):
        here = pl.ds(pl.multiple_of(z * rows + start + i * LANES, 16), LANES)
        tail_out.append(pltpu.make_async_copy(out_ref.at[here], ref, tail_sem.at[i]))
    for copy in tail_out:
        copy.start()

    units = [(SUM, 0)] + blocks
    for hop in range(2, n):
        for unit in units:
            for way in (-1, 1):
                def forward(unit=unit, way=way, hop=hop):
                    ring(unit, way, hop - 1).wait_recv()
                    ring(unit, way, hop).start()

                when(sends(unit, way, hop), forward)

    def settle(unit, way, hop):
        stays = z == 0 if way == -1 else z == n - 1
        when(jnp.logical_and(gets(unit, way, hop), stays), lambda: ring(unit, way, hop).wait_recv())

    for hop in range(1, n):
        for way in (-1, 1):
            settle((SUM, 0), way, hop)
    whole = zsum[0]
    for origin in range(1, n):
        whole = whole + zsum[origin]
    total[...] = whole
    psum[m] = whole
    for copy in tail_out:
        copy.wait()
    for c in (HEAD, BODY):
        keep(c).wait()
    for c in (MAIN, ODD, TAIL):
        for k in order:
            plane(c, k).wait_send()
    for k in order:
        plane(SUM, k).start()
    for k in order:
        plane(SUM, k).wait()
    sum_ref[...] = psum[...]

    for hop in range(1, n):
        for unit in units:
            for way in (-1, 1):
                if unit[0] != SUM:
                    settle(unit, way, hop)
                when(sends(unit, way, hop),
                     lambda unit=unit, way=way, hop=hop: ring(unit, way, hop).wait_send())


def move(weight, rank_map, n, spans, floor):
    rows, cols = weight.shape
    count = rank_map.shape[0]
    width = cols // count
    nblocks = cols // LANES
    chunks = len(spans)
    any_spec = pl.BlockSpec(memory_space=pl.ANY)
    dma = pltpu.SemaphoreType.DMA
    sent = rows * cols * 2 * (n - 1)
    return pl.pallas_call(
        functools.partial(move_kernel, n, count, spans, floor),
        in_specs=[pl.BlockSpec(memory_space=pltpu.SMEM), any_spec],
        out_specs=[any_spec] + [pl.BlockSpec(memory_space=pltpu.VMEM)] * 4,
        out_shape=[
            jax.ShapeDtypeStruct((n * rows, cols), weight.dtype),
            jax.ShapeDtypeStruct((LANES, cols), weight.dtype),
            jax.ShapeDtypeStruct((LANES, cols), weight.dtype),
            jax.ShapeDtypeStruct((LANES, cols), weight.dtype),
            jax.ShapeDtypeStruct((count, 8, LANES), jnp.float32),
        ],
        scratch_shapes=[
            pltpu.VMEM((rows, cols), weight.dtype),
            pltpu.VMEM((count, rows, width), weight.dtype),
            pltpu.VMEM((LANES, cols), jnp.bfloat16),
            pltpu.VMEM((nblocks, 8, LANES), jnp.float32),
            pltpu.VMEM((n, 8, LANES), jnp.float32),
            pltpu.VMEM((8, LANES), jnp.float32),
            pltpu.VMEM((count, 8, LANES), jnp.float32),
            dma((chunks,)),
            dma((chunks,)),
            dma((3,)),
            dma((chunks + 1, count - 1)),
            dma((chunks + 1, count - 1)),
            dma((2, n - 1, chunks + 1, count)),
            dma((2, n - 1, chunks + 1, count)),
        ],
        compiler_params=pltpu.CompilerParams(collective_id=0, has_side_effects=True, vmem_limit_bytes=VMEM_LIMIT),
        cost_estimate=pl.CostEstimate(flops=rows * cols * 8, bytes_accessed=sent * 2, transcendentals=0),
    )(rank_map, weight)


def local(n, weight, rank_map):
    rows, cols = weight.shape
    nblocks = cols // LANES
    count = rank_map.shape[0]
    total_rows = rows * n
    floor = FLOOR_RATIO / math.sqrt(total_rows)
    main = rows - 3 * LANES
    spans = ((0, main), (main, LANES), (main + LANES, 2 * LANES), (0, LANES), (LANES, main - LANES))
    ends = [(1, 0), (n - 2, n - 1)]
    even = [(a * count + m, b * count + m) for a, b in ends for m in range(0, count, 2)]

    landed, odd_own, tail_own, last_own, sums = move(weight, rank_map, n, spans, floor)
    odd_got = lax.ppermute(odd_own, ("dp", "mp"), even)
    tail_got = lax.ppermute(tail_own, "dp", ends)
    last_got = lax.ppermute(last_own, "dp", ends)
    quant, scale = quantize_all(landed, floor)
    quant, scale = fill(quant, scale, odd_got, n, rows, main, True, floor)
    quant, scale = fill(quant, scale, tail_got, n, rows, main + LANES, False, floor)
    quant, scale = fill(quant, scale, last_got, n, rows, main + 2 * LANES, False, floor)
    totals = sums[:, 0, :nblocks].reshape(-1)
    return (quant, scale.T, totals / (127.0 * math.sqrt(total_rows * LANES)))


def solution(mesh):
    n = mesh.shape["dp"]
    in_specs = (P("dp", "mp"), P())
    out_specs = (P(None, "mp"), P(None, "mp"), P())

    def body(weight, rank_map):
        return local(n, weight, rank_map)

    return jax.shard_map(body, mesh=mesh, in_specs=in_specs, out_specs=out_specs, check_vma=False)
```

```python
import functools
import math

import jax
import jax.numpy as jnp
from jax import lax
from jax.experimental import pallas as pl
from jax.experimental.pallas import tpu as pltpu
from jax.sharding import PartitionSpec as P


LANES = 128
FLOOR_RATIO = 0.25
MESH = pl.DeviceIdType.MESH
GRAIN = 32
TILE = 4 * LANES
VMEM_LIMIT = 57 * 1024 * 1024
QUANT_LIMIT = 40 * 1024 * 1024
FILL_LIMIT = 8 * 1024 * 1024


def flip(m, k):
    bit, out = 1, m
    while bit <= k:
        if k & bit:
            out = out + bit - 2 * bit * ((m // bit) % 2)
        bit *= 2
    return out


def write_spread(spread, nblocks):
    lane = lax.broadcasted_iota(jnp.int32, (LANES, LANES), 0)
    for b in range(nblocks):
        hit = jnp.logical_and(lax.rem(lane, nblocks) == b, lane < 3 * nblocks)
        spread[:, b * LANES:(b + 1) * LANES] = jnp.where(hit, 1.0, 0.0).astype(jnp.bfloat16)


def quantize_rows(x_ref, rows, spread, floor):
    nblocks = x_ref.shape[1] // LANES
    shape = (LANES, LANES)
    lane = lax.broadcasted_iota(jnp.int32, shape, 1)
    slot = lax.rem(lane, nblocks)
    peaks = jnp.zeros(shape, jnp.float32)
    for b in range(nblocks):
        peak = jnp.max(jnp.abs(x_ref[rows, b * LANES:(b + 1) * LANES]), axis=1, keepdims=True)
        peaks = jnp.where(slot == b, peak.astype(jnp.float32), peaks)
    scale = (jnp.maximum(peaks, floor) / 127.0).astype(jnp.bfloat16).astype(jnp.float32)
    yield scale
    inverse = 1.0 / scale
    high = inverse.astype(jnp.bfloat16).astype(jnp.float32)
    middle = (inverse - high).astype(jnp.bfloat16).astype(jnp.float32)
    low = inverse - high - middle
    parts = jnp.where(lane < nblocks, high, jnp.where(lane < 2 * nblocks, middle, low)).astype(jnp.bfloat16)
    for b in range(0, nblocks, 2):
        factor = jnp.dot(parts, spread[:, b * LANES:(b + 2) * LANES], preferred_element_type=jnp.float32)
        pair = x_ref[rows, b * LANES:(b + 2) * LANES].astype(jnp.float32) * factor
        yield pair.astype(jnp.bfloat16)


def quantize_tile(floor, x_ref, q_ref, s_ref, spread):
    tiles = x_ref.shape[0] // LANES

    @pl.loop(0, tiles, unroll=tiles)
    def _(t):
        rows = pl.ds(pl.multiple_of(t * LANES, LANES), LANES)
        parts = quantize_rows(x_ref, rows, spread, floor)
        s_ref[:, rows] = next(parts).T[:s_ref.shape[0]].astype(jnp.bfloat16)
        for b, part in enumerate(parts):
            q_ref[rows, b * 2 * LANES:(b + 1) * 2 * LANES] = part


def quantize_kernel(floor, x_ref, q_ref, s_ref, spread):
    @pl.when(pl.program_id(0) == 0)
    def _():
        write_spread(spread, s_ref.shape[0])

    quantize_tile(floor, x_ref, q_ref, s_ref, spread)


def quantize_all(landed, floor):
    rows, cols = landed.shape
    nblocks = cols // LANES
    tile = TILE
    return pl.pallas_call(
        functools.partial(quantize_kernel, floor),
        grid=(rows // tile,),
        in_specs=[pl.BlockSpec((tile, cols), lambda t: (t, 0))],
        out_specs=[pl.BlockSpec((tile, cols), lambda t: (t, 0)), pl.BlockSpec((nblocks, tile), lambda t: (0, t))],
        out_shape=[jax.ShapeDtypeStruct((rows, cols), jnp.bfloat16), jax.ShapeDtypeStruct((nblocks, rows), jnp.bfloat16)],
        scratch_shapes=[pltpu.VMEM((LANES, cols), jnp.bfloat16)],
        compiler_params=pltpu.CompilerParams(dimension_semantics=("arbitrary",), vmem_limit_bytes=QUANT_LIMIT),
        cost_estimate=pl.CostEstimate(flops=rows * cols * 4, bytes_accessed=rows * cols * 4, transcendentals=0),
    )(landed)


def fill_kernel(n, rows, first, even, floor, got_ref, _q, _s, q_ref, s_ref, q_v, s_v, spread, sems):
    z = lax.axis_index("dp")

    end = jnp.logical_or(z == 0, z == n - 1)
    if even:
        end = jnp.logical_and(end, lax.axis_index("mp") % 2 == 0)

    @pl.when(end)
    def _():
        write_spread(spread, s_v.shape[0])
        quantize_tile(floor, got_ref, q_v, s_v, spread)
        place = pl.ds(pl.multiple_of(jnp.where(z == 0, 1, n - 2) * rows + first, LANES), q_v.shape[0])
        copies = [pltpu.make_async_copy(q_v, q_ref.at[place], sems.at[0]),
                  pltpu.make_async_copy(s_v, s_ref.at[:, place], sems.at[1])]
        for copy in copies:
            copy.start()
        for copy in copies:
            copy.wait()


def fill(quant, scale, got, n, rows, first, even, floor):
    size, cols = got.shape
    any_spec = pl.BlockSpec(memory_space=pl.ANY)
    return pl.pallas_call(
        functools.partial(fill_kernel, n, rows, first, even, floor),
        in_specs=[pl.BlockSpec(memory_space=pltpu.VMEM), any_spec, any_spec],
        out_specs=[any_spec] * 2,
        out_shape=[jax.ShapeDtypeStruct(quant.shape, quant.dtype), jax.ShapeDtypeStruct(scale.shape, scale.dtype)],
        input_output_aliases={1: 0, 2: 1},
        scratch_shapes=[
            pltpu.VMEM((size, cols), quant.dtype),
            pltpu.VMEM((scale.shape[0], size), scale.dtype),
            pltpu.VMEM((LANES, cols), jnp.bfloat16),
            pltpu.SemaphoreType.DMA((2,)),
        ],
        compiler_params=pltpu.CompilerParams(vmem_limit_bytes=FILL_LIMIT),
        cost_estimate=pl.CostEstimate(flops=size * cols * 4, bytes_accessed=size * cols * 4, transcendentals=0),
    )(got, quant, scale)


def move_kernel(n, count, spans, floor, map_ref, w_ref, out_ref, odd_ref, tail_ref, last_ref, sum_ref,
                stage, perm, spread, acc, zsum, total, psum,
                load_sem, own_sem, tail_sem, a_send, a_recv, z_send, z_recv, p_send, p_recv, s_send, s_recv):
    z = lax.axis_index("dp")
    m = lax.axis_index("mp")
    rows, width = perm.shape[1:]
    group = width // LANES
    nblocks = count * group
    MAIN, ODD, TAIL, HEAD, BODY, SUM = range(6)
    order = sorted(range(1, count), key=lambda k: (bin(k).count("1"), k))

    def when(cond, act):
        @pl.when(cond)
        def _():
            act()

    loads = {c: pltpu.make_async_copy(w_ref.at[pl.ds(*spans[c])], stage.at[pl.ds(*spans[c])], load_sem.at[c])
             for c in (HEAD, BODY, ODD, TAIL)}
    for load in loads.values():
        load.start()

    barrier = pltpu.get_barrier_semaphore()
    for k in range(1, count):
        pl.semaphore_signal(barrier, inc=1, device_id=(z, flip(m, k)), device_id_type=MESH)
    when(z > 0, lambda: pl.semaphore_signal(barrier, inc=1, device_id=(z - 1, m), device_id_type=MESH))
    when(z < n - 1, lambda: pl.semaphore_signal(barrier, inc=1, device_id=(z + 1, m), device_id_type=MESH))
    beside = jnp.where(z > 0, 1, 0) + jnp.where(z < n - 1, 1, 0)

    holds = [[map_ref[j] == r for j in range(count)] for r in range(count)]

    def arrange(c):
        start, size = spans[c]
        loads[c].wait()

        @pl.loop(0, size // GRAIN)
        def _(t):
            here = pl.ds(pl.multiple_of(start + t * GRAIN, GRAIN), GRAIN)
            for i in range(group):
                first = i * count
                blocks = [stage[here, (first + j) * LANES:(first + j + 1) * LANES] for j in range(count)]
                for r in range(count):
                    block = blocks[0]
                    for j in range(1, count):
                        block = jnp.where(holds[r][j], blocks[j], block)
                    perm[r, here, i * LANES:(i + 1) * LANES] = block

    blocks = [(HEAD, 0), (BODY, 0)] + [(MAIN, k) for k in order] + [(c, k) for c in (ODD, TAIL) for k in [0] + order]
    slots = {unit: slot for slot, unit in enumerate(blocks)}

    def place(origin, c, src):
        start, size = spans[c]
        return out_ref.at[pl.ds(pl.multiple_of(origin * rows + start, 16), size),
                          pl.ds(pl.multiple_of(src * width, LANES), width)]

    def own(c):
        return perm.at[m, pl.ds(*spans[c])]

    def plane(c, k):
        peer = flip(m, k)
        if c == SUM:
            src, dst, send, recv = total, psum.at[m], p_send.at[k - 1], p_recv.at[k - 1]
        else:
            src, dst = perm.at[peer, pl.ds(*spans[c])], place(z, c, m)
            send, recv = a_send.at[c], a_recv.at[c, k - 1]
        return pltpu.make_async_remote_copy(
            src_ref=src, dst_ref=dst, send_sem=send, recv_sem=recv, device_id=(z, peer), device_id_type=MESH)

    def ring(unit, way, hop, got=False):
        c, k = unit
        origin = z + way * -hop if got else z - way * (hop - 1)
        w = 0 if way == 1 else 1
        if c == SUM:
            src = dst = zsum.at[origin]
            send, recv = s_send.at[w, hop - 1], s_recv.at[origin]
        else:
            dst = place(origin, c, flip(m, k))
            src = own(c) if hop == 1 and k == 0 and not got else dst
            send, recv = z_send.at[w, hop - 1, min(c, HEAD) % HEAD], z_recv.at[origin, slots[unit]]
        return pltpu.make_async_remote_copy(
            src_ref=src, dst_ref=dst, send_sem=send, recv_sem=recv,
            device_id=(z + way, m), device_id_type=MESH)

    def sent(refs, sem):
        pltpu.make_async_copy(refs, refs, sem).wait()

    def kept(unit, hop):
        return {TAIL: 1, ODD: 1 - m % 2}.get(unit[0], 0) if hop == 1 else 0

    def sends(unit, way, hop):
        low = kept(unit, hop)
        if way == -1:
            return jnp.logical_and(z > low, z + hop - 1 <= n - 1)
        return jnp.logical_and(z < n - 1 - low, z - (hop - 1) >= 0)

    def gets(unit, way, hop):
        low = kept(unit, hop)
        if way == -1:
            return jnp.logical_and(z >= low, z + hop <= n - 1)
        return jnp.logical_and(z <= n - 1 - low, z - hop >= 0)

    def start_ring(unit):
        for way in (-1, 1):
            when(sends(unit, way, 1), lambda way=way: ring(unit, way, 1).start())

    def keep(c):
        return pltpu.make_async_copy(own(c), place(z, c, m), own_sem.at[c])

    def send_own(c):
        start_ring((c, 0))
        keep(c).start()

    def send_plane(c):
        for k in order:
            plane(c, k).start()

    def add_up(first, size):
        @pl.loop(0, size // LANES)
        def _(t):
            parts = quantize_rows(stage, pl.ds(pl.multiple_of(first + t * LANES, LANES), LANES), spread, floor)
            next(parts)
            for b, part in enumerate(parts):
                both = part.astype(jnp.float32)
                for i in range(2):
                    one = both[:, i * LANES:(i + 1) * LANES].reshape(LANES // 8, 8, LANES)
                    acc[2 * b + i] += jnp.sum(one, axis=0)

    arrange(HEAD)
    pl.semaphore_wait(barrier, count - 1 + beside)
    send_own(HEAD)
    arrange(BODY)
    send_own(BODY)
    arrange(ODD)
    send_plane(MAIN)
    arrange(TAIL)
    send_own(ODD)
    send_plane(ODD)
    acc[...] = jnp.zeros_like(acc)
    write_spread(spread, nblocks)
    add_up(*spans[HEAD])
    send_own(TAIL)
    send_plane(TAIL)
    add_up(spans[HEAD][1], rows - spans[HEAD][1])

    sums = jnp.sum(jnp.sum(acc[...], axis=1), axis=1, keepdims=True)
    row = lax.broadcasted_iota(jnp.int32, (nblocks, LANES), 0)
    col = lax.broadcasted_iota(jnp.int32, (nblocks, LANES), 1)
    line = jnp.sum(jnp.where(row == col, sums, 0.0), axis=0, keepdims=True)
    zsum[z] = jnp.broadcast_to(line, zsum.shape[1:])

    for c, k in blocks:
        if k > 0:
            plane(c, k).wait_recv()
            start_ring((c, k))
            if (c, k) == (MAIN, order[0]):
                start_ring((SUM, 0))

    keep(ODD).wait()
    keep(TAIL).wait()
    start = spans[ODD][0]
    size = rows - start
    tail = pl.ds(pl.multiple_of(z * rows + start, 16), size)
    tail_in = pltpu.make_async_copy(out_ref.at[tail], stage.at[pl.ds(0, size)], tail_sem.at[0])
    tail_in.start()
    tail_in.wait()
    tail_out = [pltpu.make_async_copy(stage.at[pl.ds(i * LANES, LANES)], ref, tail_sem.at[i + 1])
                for i, ref in enumerate((odd_ref, tail_ref, last_ref))]
    for copy in tail_out:
        copy.start()

    units = [(SUM, 0)] + blocks
    for hop in range(2, n):
        for unit in units:
            for way in (-1, 1):
                def forward(unit=unit, way=way, hop=hop):
                    ring(unit, way, hop - 1, True).wait_recv()
                    ring(unit, way, hop).start()

                when(sends(unit, way, hop), forward)

    def settle(unit, way, hop):
        stays = z == 0 if way == -1 else z == n - 1
        when(jnp.logical_and(gets(unit, way, hop), stays), lambda: ring(unit, way, hop, True).wait_recv())

    for hop in range(1, n):
        for way in (-1, 1):
            settle((SUM, 0), way, hop)
    whole = zsum[0]
    for origin in range(1, n):
        whole = whole + zsum[origin]
    total[...] = whole
    psum[m] = whole
    for copy in tail_out:
        copy.wait()
    for c in (HEAD, BODY):
        keep(c).wait()
    for c in (MAIN, ODD, TAIL):
        sent(perm.at[pl.ds(0, count - 1), pl.ds(*spans[c])], a_send.at[c])
    for k in order:
        plane(SUM, k).start()
    for k in order:
        plane(SUM, k).wait()
    sums_out = pltpu.make_async_copy(psum, sum_ref, tail_sem.at[0])
    sums_out.start()
    for hop in range(1, n):
        for way in (-1, 1):
            when(sends((SUM, 0), way, hop), lambda way=way, hop=hop: ring((SUM, 0), way, hop).wait_send())
    sums_out.wait()

    for hop in range(1, n):
        for unit in blocks:
            for way in (-1, 1):
                settle(unit, way, hop)
        for c in (MAIN, ODD, TAIL):
            for way in (-1, 1):
                w = 0 if way == 1 else 1
                when(sends((c, 0), way, hop),
                     lambda c=c, w=w, hop=hop: sent(out_ref.at[pl.ds(*spans[c])], z_send.at[w, hop - 1, c]))


def move(weight, rank_map, n, spans, floor):
    rows, cols = weight.shape
    count = rank_map.shape[0]
    width = cols // count
    nblocks = cols // LANES
    chunks = len(spans)
    any_spec = pl.BlockSpec(memory_space=pl.ANY)
    dma = pltpu.SemaphoreType.DMA
    sent = rows * cols * 2 * (n - 1)
    return pl.pallas_call(
        functools.partial(move_kernel, n, count, spans, floor),
        in_specs=[pl.BlockSpec(memory_space=pltpu.SMEM), any_spec],
        out_specs=[any_spec] + [any_spec] * 4,
        out_shape=[
            jax.ShapeDtypeStruct((n * rows, cols), weight.dtype),
            jax.ShapeDtypeStruct((LANES, cols), weight.dtype),
            jax.ShapeDtypeStruct((LANES, cols), weight.dtype),
            jax.ShapeDtypeStruct((LANES, cols), weight.dtype),
            jax.ShapeDtypeStruct((count, 8, LANES), jnp.float32),
        ],
        scratch_shapes=[
            pltpu.VMEM((rows, cols), weight.dtype),
            pltpu.VMEM((count, rows, width), weight.dtype),
            pltpu.VMEM((LANES, cols), jnp.bfloat16),
            pltpu.VMEM((nblocks, 8, LANES), jnp.float32),
            pltpu.VMEM((n, 8, LANES), jnp.float32),
            pltpu.VMEM((8, LANES), jnp.float32),
            pltpu.VMEM((count, 8, LANES), jnp.float32),
            dma((chunks,)),
            dma((chunks,)),
            dma((4,)),
            dma((3,)),
            dma((3, count - 1)),
            dma((2, n - 1, 3)),
            dma((n, 3 * count + 1)),
            dma((count - 1,)),
            dma((count - 1,)),
            dma((2, n - 1)),
            dma((n,)),
        ],
        compiler_params=pltpu.CompilerParams(collective_id=0, has_side_effects=True, vmem_limit_bytes=VMEM_LIMIT),
        cost_estimate=pl.CostEstimate(flops=rows * cols * 8, bytes_accessed=sent * 2, transcendentals=0),
    )(rank_map, weight)


def local(n, weight, rank_map):
    rows, cols = weight.shape
    nblocks = cols // LANES
    count = rank_map.shape[0]
    total_rows = rows * n
    floor = FLOOR_RATIO / math.sqrt(total_rows)
    main = rows - 3 * LANES
    spans = ((0, main), (main, LANES), (main + LANES, 2 * LANES), (0, LANES), (LANES, main - LANES))
    ends = [(1, 0), (n - 2, n - 1)]
    even = [(a * count + m, b * count + m) for a, b in ends for m in range(0, count, 2)]

    landed, odd_own, tail_own, last_own, sums = move(weight, rank_map, n, spans, floor)
    odd_got = lax.ppermute(odd_own, ("dp", "mp"), even)
    tail_got = lax.ppermute(tail_own, "dp", ends)
    last_got = lax.ppermute(last_own, "dp", ends)
    quant, scale = quantize_all(landed, floor)
    quant, scale = fill(quant, scale, odd_got, n, rows, main, True, floor)
    quant, scale = fill(quant, scale, tail_got, n, rows, main + LANES, False, floor)
    quant, scale = fill(quant, scale, last_got, n, rows, main + 2 * LANES, False, floor)
    totals = sums[:, 0, :nblocks].reshape(-1)
    return (quant, scale.T, totals / (127.0 * math.sqrt(total_rows * LANES)))


def solution(mesh):
    n = mesh.shape["dp"]
    in_specs = (P("dp", "mp"), P())
    out_specs = (P(None, "mp"), P(None, "mp"), P())

    def body(weight, rank_map):
        return local(n, weight, rank_map)

    return jax.shard_map(body, mesh=mesh, in_specs=in_specs, out_specs=out_specs, check_vma=False)
```

```python
import functools
import math

import jax
import jax.numpy as jnp
from jax import lax
from jax.experimental import pallas as pl
from jax.experimental.pallas import tpu as pltpu
from jax.sharding import PartitionSpec as P


LANES = 128
FLOOR_RATIO = 0.25
MESH = pl.DeviceIdType.MESH
GRAIN = 32
TILE = 4 * LANES
VMEM_LIMIT = 57 * 1024 * 1024
QUANT_LIMIT = 40 * 1024 * 1024
FILL_LIMIT = 8 * 1024 * 1024


def flip(m, k):
    bit, out = 1, m
    while bit <= k:
        if k & bit:
            out = out + bit - 2 * bit * ((m // bit) % 2)
        bit *= 2
    return out


def write_spread(spread, nblocks):
    lane = lax.broadcasted_iota(jnp.int32, (LANES, LANES), 0)
    for b in range(nblocks):
        hit = jnp.logical_and(lax.rem(lane, nblocks) == b, lane < 3 * nblocks)
        spread[:, b * LANES:(b + 1) * LANES] = jnp.where(hit, 1.0, 0.0).astype(jnp.bfloat16)


def quantize_rows(x_ref, rows, spread, floor):
    nblocks = x_ref.shape[1] // LANES
    shape = (LANES, LANES)
    lane = lax.broadcasted_iota(jnp.int32, shape, 1)
    slot = lax.rem(lane, nblocks)
    peaks = jnp.zeros(shape, jnp.float32)
    for b in range(nblocks):
        peak = jnp.max(jnp.abs(x_ref[rows, b * LANES:(b + 1) * LANES]), axis=1, keepdims=True)
        peaks = jnp.where(slot == b, peak.astype(jnp.float32), peaks)
    scale = (jnp.maximum(peaks, floor) / 127.0).astype(jnp.bfloat16).astype(jnp.float32)
    yield scale
    inverse = 1.0 / scale
    high = inverse.astype(jnp.bfloat16).astype(jnp.float32)
    middle = (inverse - high).astype(jnp.bfloat16).astype(jnp.float32)
    low = inverse - high - middle
    parts = jnp.where(lane < nblocks, high, jnp.where(lane < 2 * nblocks, middle, low)).astype(jnp.bfloat16)
    for b in range(0, nblocks, 2):
        factor = jnp.dot(parts, spread[:, b * LANES:(b + 2) * LANES], preferred_element_type=jnp.float32)
        pair = x_ref[rows, b * LANES:(b + 2) * LANES].astype(jnp.float32) * factor
        yield pair.astype(jnp.bfloat16)


def quantize_tile(floor, x_ref, q_ref, s_ref, spread):
    tiles = x_ref.shape[0] // LANES

    @pl.loop(0, tiles, unroll=tiles)
    def _(t):
        rows = pl.ds(pl.multiple_of(t * LANES, LANES), LANES)
        parts = quantize_rows(x_ref, rows, spread, floor)
        s_ref[:, rows] = next(parts).T[:s_ref.shape[0]].astype(jnp.bfloat16)
        for b, part in enumerate(parts):
            q_ref[rows, b * 2 * LANES:(b + 1) * 2 * LANES] = part


def quantize_kernel(floor, x_ref, q_ref, s_ref, spread):
    @pl.when(pl.program_id(0) == 0)
    def _():
        write_spread(spread, s_ref.shape[0])

    quantize_tile(floor, x_ref, q_ref, s_ref, spread)


def quantize_all(landed, floor):
    rows, cols = landed.shape
    nblocks = cols // LANES
    tile = TILE
    return pl.pallas_call(
        functools.partial(quantize_kernel, floor),
        grid=(rows // tile,),
        in_specs=[pl.BlockSpec((tile, cols), lambda t: (t, 0))],
        out_specs=[pl.BlockSpec((tile, cols), lambda t: (t, 0)), pl.BlockSpec((nblocks, tile), lambda t: (0, t))],
        out_shape=[jax.ShapeDtypeStruct((rows, cols), jnp.bfloat16), jax.ShapeDtypeStruct((nblocks, rows), jnp.bfloat16)],
        scratch_shapes=[pltpu.VMEM((LANES, cols), jnp.bfloat16)],
        compiler_params=pltpu.CompilerParams(dimension_semantics=("arbitrary",), vmem_limit_bytes=QUANT_LIMIT),
        cost_estimate=pl.CostEstimate(flops=rows * cols * 4, bytes_accessed=rows * cols * 4, transcendentals=0),
    )(landed)


def fill_kernel(n, rows, first, even, floor, got_ref, _q, _s, q_ref, s_ref, q_v, s_v, spread, sems):
    z = lax.axis_index("dp")

    end = jnp.logical_or(z == 0, z == n - 1)
    if even:
        end = jnp.logical_and(end, lax.axis_index("mp") % 2 == 0)

    @pl.when(end)
    def _():
        write_spread(spread, s_v.shape[0])
        size, half = q_v.shape[1:]
        place = pl.ds(pl.multiple_of(jnp.where(z == 0, 1, n - 2) * rows + first, LANES), size)
        parts = quantize_rows(got_ref, pl.ds(0, size), spread, floor)
        s_v[...] = next(parts).T[:s_v.shape[0]].astype(jnp.bfloat16)
        copies = [pltpu.make_async_copy(s_v, s_ref.at[:, place], sems.at[2])]
        copies[0].start()
        wide = 2 * LANES
        for side in range(2):
            for col in range(0, half, wide):
                q_v[side, :, col:col + wide] = next(parts)
            copies.append(pltpu.make_async_copy(q_v.at[side], q_ref.at[place, pl.ds(side * half, half)], sems.at[side]))
            copies[-1].start()
        for copy in copies:
            copy.wait()


def fill(quant, scale, got, n, rows, first, even, floor):
    size, cols = got.shape
    any_spec = pl.BlockSpec(memory_space=pl.ANY)
    return pl.pallas_call(
        functools.partial(fill_kernel, n, rows, first, even, floor),
        in_specs=[pl.BlockSpec(memory_space=pltpu.VMEM), any_spec, any_spec],
        out_specs=[any_spec] * 2,
        out_shape=[jax.ShapeDtypeStruct(quant.shape, quant.dtype), jax.ShapeDtypeStruct(scale.shape, scale.dtype)],
        input_output_aliases={1: 0, 2: 1},
        scratch_shapes=[
            pltpu.VMEM((2, size, cols // 2), quant.dtype),
            pltpu.VMEM((scale.shape[0], size), scale.dtype),
            pltpu.VMEM((LANES, cols), jnp.bfloat16),
            pltpu.SemaphoreType.DMA((3,)),
        ],
        compiler_params=pltpu.CompilerParams(vmem_limit_bytes=FILL_LIMIT),
        cost_estimate=pl.CostEstimate(flops=size * cols * 4, bytes_accessed=size * cols * 4, transcendentals=0),
    )(got, quant, scale)


def move_kernel(n, count, spans, floor, map_ref, w_ref, out_ref, odd_ref, tail_ref, last_ref, sum_ref,
                stage, perm, spread, acc, zsum, total, psum,
                load_sem, own_sem, tail_sem, a_send, a_recv, z_send, z_recv, p_send, p_recv, s_send, s_recv):
    z = lax.axis_index("dp")
    m = lax.axis_index("mp")
    rows, width = perm.shape[1:]
    group = width // LANES
    nblocks = count * group
    MAIN, ODD, TAIL, HEAD, BODY, SUM = range(6)
    order = sorted(range(1, count), key=lambda k: (bin(k).count("1"), k))

    def when(cond, act):
        @pl.when(cond)
        def _():
            act()

    loads = {c: pltpu.make_async_copy(w_ref.at[pl.ds(*spans[c])], stage.at[pl.ds(*spans[c])], load_sem.at[c])
             for c in (HEAD, BODY, ODD, TAIL)}
    for load in loads.values():
        load.start()

    barrier = pltpu.get_barrier_semaphore()
    for k in range(1, count):
        pl.semaphore_signal(barrier, inc=1, device_id=(z, flip(m, k)), device_id_type=MESH)
    when(z > 0, lambda: pl.semaphore_signal(barrier, inc=1, device_id=(z - 1, m), device_id_type=MESH))
    when(z < n - 1, lambda: pl.semaphore_signal(barrier, inc=1, device_id=(z + 1, m), device_id_type=MESH))
    beside = jnp.where(z > 0, 1, 0) + jnp.where(z < n - 1, 1, 0)

    holds = [[map_ref[j] == r for j in range(count)] for r in range(count)]

    def arrange(c):
        start, size = spans[c]
        loads[c].wait()

        @pl.loop(0, size // GRAIN)
        def _(t):
            here = pl.ds(pl.multiple_of(start + t * GRAIN, GRAIN), GRAIN)
            for i in range(group):
                first = i * count
                blocks = [stage[here, (first + j) * LANES:(first + j + 1) * LANES] for j in range(count)]
                for r in range(count):
                    block = blocks[0]
                    for j in range(1, count):
                        block = jnp.where(holds[r][j], blocks[j], block)
                    perm[r, here, i * LANES:(i + 1) * LANES] = block

    blocks = [(HEAD, 0), (BODY, 0)] + [(MAIN, k) for k in order] + [(c, k) for c in (ODD, TAIL) for k in [0] + order]
    slots = {unit: slot for slot, unit in enumerate(blocks)}

    def place(origin, c, src):
        start, size = spans[c]
        return out_ref.at[pl.ds(pl.multiple_of(origin * rows + start, 16), size),
                          pl.ds(pl.multiple_of(src * width, LANES), width)]

    def own(c):
        return perm.at[m, pl.ds(*spans[c])]

    def plane(c, k):
        peer = flip(m, k)
        if c == SUM:
            src, dst, send, recv = total, psum.at[m], p_send.at[k - 1], p_recv.at[k - 1]
        else:
            src, dst = perm.at[peer, pl.ds(*spans[c])], place(z, c, m)
            send, recv = a_send.at[c], a_recv.at[c, k - 1]
        return pltpu.make_async_remote_copy(
            src_ref=src, dst_ref=dst, send_sem=send, recv_sem=recv, device_id=(z, peer), device_id_type=MESH)

    def ring(unit, way, hop, got=False):
        c, k = unit
        origin = z + way * -hop if got else z - way * (hop - 1)
        w = 0 if way == 1 else 1
        if c == SUM:
            src = dst = zsum.at[origin]
            send, recv = s_send.at[w, hop - 1], s_recv.at[origin]
        else:
            dst = place(origin, c, flip(m, k))
            src = own(c) if hop == 1 and k == 0 and not got else dst
            send, recv = z_send.at[w, hop - 1, min(c, HEAD) % HEAD], z_recv.at[origin, slots[unit]]
        return pltpu.make_async_remote_copy(
            src_ref=src, dst_ref=dst, send_sem=send, recv_sem=recv,
            device_id=(z + way, m), device_id_type=MESH)

    def sent(refs, sem):
        pltpu.make_async_copy(refs, refs, sem).wait()

    def kept(unit, hop):
        return {TAIL: 1, ODD: 1 - m % 2}.get(unit[0], 0) if hop == 1 else 0

    def sends(unit, way, hop):
        low = kept(unit, hop)
        if way == -1:
            return jnp.logical_and(z > low, z + hop - 1 <= n - 1)
        return jnp.logical_and(z < n - 1 - low, z - (hop - 1) >= 0)

    def gets(unit, way, hop):
        low = kept(unit, hop)
        if way == -1:
            return jnp.logical_and(z >= low, z + hop <= n - 1)
        return jnp.logical_and(z <= n - 1 - low, z - hop >= 0)

    def start_ring(unit):
        for way in (-1, 1):
            when(sends(unit, way, 1), lambda way=way: ring(unit, way, 1).start())

    def keep(c):
        return pltpu.make_async_copy(own(c), place(z, c, m), own_sem.at[c])

    def send_own(c):
        start_ring((c, 0))
        keep(c).start()

    def send_plane(c):
        for k in order:
            plane(c, k).start()

    def add_up(first, size):
        @pl.loop(0, size // LANES)
        def _(t):
            parts = quantize_rows(stage, pl.ds(pl.multiple_of(first + t * LANES, LANES), LANES), spread, floor)
            next(parts)
            for b, part in enumerate(parts):
                both = part.astype(jnp.float32)
                for i in range(2):
                    one = both[:, i * LANES:(i + 1) * LANES].reshape(LANES // 8, 8, LANES)
                    acc[2 * b + i] += jnp.sum(one, axis=0)

    arrange(HEAD)
    pl.semaphore_wait(barrier, count - 1 + beside)
    send_own(HEAD)
    arrange(BODY)
    send_own(BODY)
    arrange(ODD)
    send_plane(MAIN)
    arrange(TAIL)
    send_own(ODD)
    send_plane(ODD)
    acc[...] = jnp.zeros_like(acc)
    write_spread(spread, nblocks)
    add_up(*spans[HEAD])
    send_own(TAIL)
    send_plane(TAIL)
    add_up(spans[HEAD][1], rows - spans[HEAD][1])

    sums = jnp.sum(jnp.sum(acc[...], axis=1), axis=1, keepdims=True)
    row = lax.broadcasted_iota(jnp.int32, (nblocks, LANES), 0)
    col = lax.broadcasted_iota(jnp.int32, (nblocks, LANES), 1)
    line = jnp.sum(jnp.where(row == col, sums, 0.0), axis=0, keepdims=True)
    zsum[z] = jnp.broadcast_to(line, zsum.shape[1:])

    for c, k in blocks:
        if k > 0:
            plane(c, k).wait_recv()
            start_ring((c, k))
            if (c, k) == (MAIN, order[0]):
                start_ring((SUM, 0))

    keep(ODD).wait()
    keep(TAIL).wait()
    start = spans[ODD][0]
    size = rows - start
    tail = pl.ds(pl.multiple_of(z * rows + start, 16), size)
    tail_in = pltpu.make_async_copy(out_ref.at[tail], stage.at[pl.ds(0, size)], tail_sem.at[0])
    tail_in.start()
    tail_in.wait()
    tail_out = [pltpu.make_async_copy(stage.at[pl.ds(i * LANES, LANES)], ref, tail_sem.at[i + 1])
                for i, ref in enumerate((odd_ref, tail_ref, last_ref))]
    for copy in tail_out:
        copy.start()

    units = [(SUM, 0)] + blocks
    for hop in range(2, n):
        for unit in units:
            for way in (-1, 1):
                def forward(unit=unit, way=way, hop=hop):
                    ring(unit, way, hop - 1, True).wait_recv()
                    ring(unit, way, hop).start()

                when(sends(unit, way, hop), forward)

    def settle(unit, way, hop):
        stays = z == 0 if way == -1 else z == n - 1
        when(jnp.logical_and(gets(unit, way, hop), stays), lambda: ring(unit, way, hop, True).wait_recv())

    for hop in range(1, n):
        for way in (-1, 1):
            settle((SUM, 0), way, hop)
    whole = zsum[0]
    for origin in range(1, n):
        whole = whole + zsum[origin]
    total[...] = whole
    psum[m] = whole
    for copy in tail_out:
        copy.wait()
    for c in (HEAD, BODY):
        keep(c).wait()
    for c in (MAIN, ODD, TAIL):
        sent(perm.at[pl.ds(0, count - 1), pl.ds(*spans[c])], a_send.at[c])
    for k in order:
        plane(SUM, k).start()
    for k in order:
        plane(SUM, k).wait()
    sums_out = pltpu.make_async_copy(psum, sum_ref, tail_sem.at[0])
    sums_out.start()
    for hop in range(1, n):
        for way in (-1, 1):
            when(sends((SUM, 0), way, hop), lambda way=way, hop=hop: ring((SUM, 0), way, hop).wait_send())
    sums_out.wait()

    for hop in range(1, n):
        for unit in blocks:
            for way in (-1, 1):
                settle(unit, way, hop)
        for c in (MAIN, ODD, TAIL):
            for way in (-1, 1):
                w = 0 if way == 1 else 1
                when(sends((c, 0), way, hop),
                     lambda c=c, w=w, hop=hop: sent(out_ref.at[pl.ds(*spans[c])], z_send.at[w, hop - 1, c]))


def move(weight, rank_map, n, spans, floor):
    rows, cols = weight.shape
    count = rank_map.shape[0]
    width = cols // count
    nblocks = cols // LANES
    chunks = len(spans)
    any_spec = pl.BlockSpec(memory_space=pl.ANY)
    dma = pltpu.SemaphoreType.DMA
    sent = rows * cols * 2 * (n - 1)
    return pl.pallas_call(
        functools.partial(move_kernel, n, count, spans, floor),
        in_specs=[pl.BlockSpec(memory_space=pltpu.SMEM), any_spec],
        out_specs=[any_spec] + [any_spec] * 4,
        out_shape=[
            jax.ShapeDtypeStruct((n * rows, cols), weight.dtype),
            jax.ShapeDtypeStruct((LANES, cols), weight.dtype),
            jax.ShapeDtypeStruct((LANES, cols), weight.dtype),
            jax.ShapeDtypeStruct((LANES, cols), weight.dtype),
            jax.ShapeDtypeStruct((count, 8, LANES), jnp.float32),
        ],
        scratch_shapes=[
            pltpu.VMEM((rows, cols), weight.dtype),
            pltpu.VMEM((count, rows, width), weight.dtype),
            pltpu.VMEM((LANES, cols), jnp.bfloat16),
            pltpu.VMEM((nblocks, 8, LANES), jnp.float32),
            pltpu.VMEM((n, 8, LANES), jnp.float32),
            pltpu.VMEM((8, LANES), jnp.float32),
            pltpu.VMEM((count, 8, LANES), jnp.float32),
            dma((chunks,)),
            dma((chunks,)),
            dma((4,)),
            dma((3,)),
            dma((3, count - 1)),
            dma((2, n - 1, 3)),
            dma((n, 3 * count + 1)),
            dma((count - 1,)),
            dma((count - 1,)),
            dma((2, n - 1)),
            dma((n,)),
        ],
        compiler_params=pltpu.CompilerParams(collective_id=0, has_side_effects=True, vmem_limit_bytes=VMEM_LIMIT),
        cost_estimate=pl.CostEstimate(flops=rows * cols * 8, bytes_accessed=sent * 2, transcendentals=0),
    )(rank_map, weight)


def local(n, weight, rank_map):
    rows, cols = weight.shape
    nblocks = cols // LANES
    count = rank_map.shape[0]
    total_rows = rows * n
    floor = FLOOR_RATIO / math.sqrt(total_rows)
    main = rows - 3 * LANES
    spans = ((0, main), (main, LANES), (main + LANES, 2 * LANES), (0, LANES), (LANES, main - LANES))
    ends = [(1, 0), (n - 2, n - 1)]
    even = [(a * count + m, b * count + m) for a, b in ends for m in range(0, count, 2)]

    landed, odd_own, tail_own, last_own, sums = move(weight, rank_map, n, spans, floor)
    odd_got = lax.ppermute(odd_own, ("dp", "mp"), even)
    tail_got = lax.ppermute(tail_own, "dp", ends)
    last_got = lax.ppermute(last_own, "dp", ends)
    quant, scale = quantize_all(landed, floor)
    quant, scale = fill(quant, scale, odd_got, n, rows, main, True, floor)
    quant, scale = fill(quant, scale, tail_got, n, rows, main + LANES, False, floor)
    quant, scale = fill(quant, scale, last_got, n, rows, main + 2 * LANES, False, floor)
    totals = sums[:, 0, :nblocks].reshape(-1)
    return (quant, scale.T, totals / (127.0 * math.sqrt(total_rows * LANES)))


def solution(mesh):
    n = mesh.shape["dp"]
    in_specs = (P("dp", "mp"), P())
    out_specs = (P(None, "mp"), P(None, "mp"), P())

    def body(weight, rank_map):
        return local(n, weight, rank_map)

    return jax.shard_map(body, mesh=mesh, in_specs=in_specs, out_specs=out_specs, check_vma=False)
```
